32 devices in a mesh: rep: 8 (over y, x, core), fsdp: 4 (over z).
Axes of the slice: x: 2, y: 2, z: 4, core: 2. Of those that a mesh axis runs over, the one named last changes fastest.
Arguments:
- codes: bfloat16 [8, 4096, 1024], P('rep', 'fsdp'), may hold values from -127 to 127
- block_scales: float32 [8, 4096, 8], P('rep', 'fsdp'), may hold values from 0.002 to 0.02
- params: bfloat16 [4096, 1024], P('fsdp'), may hold values from -6 to 6
- momentum: bfloat16 [4096, 1024], P('fsdp'), may hold values from -3 to 3
Outputs:
- new_params: bfloat16 [4096, 1024], replicated
- new_momentum: bfloat16 [4096, 1024], P('fsdp')
The draws below stay inside these ranges and needn't reach their ends.
All inputs are finite; a program needn't handle non-finite values.
Results may differ from the reference program's by a relative error of at most 0.006.
Values may be sent and summed in bfloat16 or wider, within the bound.
No kernel may reach another device: no remote copies, remote signals or barrier semaphores. Data moves between devices by JAX's collectives and lax.ppermute only.
A program may use at most 64 MiB of HBM per device.

```python
import math
import jax
import jax.numpy as jnp
from jax import lax

D = 4096
KV = 1024
BLOCK = 128
REP = 8
N_REP = 8


def levels(rng, extent, shards, low, top_value):
    level, own = 1.0, jax.random.fold_in(rng, 6)
    for dim, shards_of in shards:
        steps = jnp.exp(jax.random.uniform(jax.random.fold_in(own, dim), (shards_of,), jnp.float32, low / len(shards), top_value / len(shards)))
        level = level * jnp.repeat(steps, extent[dim] // shards_of).reshape([-1 if axis == dim else 1 for axis in range(len(extent))])
    return level


def centred(key, extent, scale, limit, split=(), dtype=jnp.bfloat16):
    array = jax.random.normal(key, extent, jnp.float32) * scale
    if len(split) > 0:
        array = levels(key, extent, split, -0.22, 0.18) * array
    return jnp.clip(array, min=-limit, max=limit).astype(dtype)


def setup_inputs(seed: int = 0) -> dict:
    key_of = jax.random.split(jax.random.key(seed), 5)
    return {
        "codes": centred(key_of[0], (REP, D, KV), 40.0, 127.0, ((0, 8), (1, 4))),
        "block_scales": jnp.clip(jnp.exp(math.log(0.02) - 2.30258502 * jax.random.uniform(key_of[1], (REP, D, KV // BLOCK), jnp.float32) ** levels(key_of[1], (REP, D, KV // BLOCK), ((0, 8), (1, 4)), -0.2, 0.2)), 0.002, 0.02),
        "params": centred(key_of[2], (D, KV), 1.0, 6.0, ((0, 4),)),
        "momentum": centred(key_of[3], (D, KV), 0.5, 3.0, ((0, 4),)),
    }


def reference(codes, block_scales, params, momentum):
    def accumulate(total, pair):
        code_block, scale_block = pair
        pieces = code_block.astype(jnp.float32).reshape(D, KV // BLOCK, BLOCK) * scale_block[:, :, None]
        return total + pieces.reshape(D, KV), None

    total, unused = lax.scan(accumulate, jnp.zeros((D, KV), jnp.float32), (codes, block_scales))
    delta = total / N_REP
    moment = 0.9 * momentum.astype(jnp.float32) + delta
    new_params = (params.astype(jnp.float32) - 0.7 * (delta + 0.9 * moment)).astype(jnp.bfloat16)
    return new_params, moment.astype(jnp.bfloat16)
```

```python
import functools

import jax
import jax.numpy as jnp
import numpy as np
from jax import lax
from jax.experimental import pallas as pl
from jax.experimental.pallas import tpu as pltpu
from jax.sharding import PartitionSpec as P

LANES = 128
PARAMS = pltpu.CompilerParams(vmem_limit_bytes=12 << 20)


def dequantize(code_rows, scale_rows):
    count, width = code_rows.shape
    pieces = (
        code_rows.astype(jnp.float32).reshape(count, width // LANES, LANES)
        * scale_rows[:, :, None]
    )
    return pieces.reshape(count, width)


def step_of(total, params, momentum, replicas):
    delta = total * (1.0 / replicas)
    moment = 0.9 * momentum.astype(jnp.float32) + delta
    updated = params.astype(jnp.float32) - 0.7 * (delta + 0.9 * moment)
    return updated.astype(jnp.bfloat16), moment.astype(jnp.bfloat16)


def general(codes, block_scales, params, momentum):
    replicas = lax.axis_size("rep")
    term = dequantize(codes[0], block_scales[0]).astype(jnp.bfloat16)
    share = lax.psum_scatter(term, "rep", scatter_dimension=0, tiled=True)
    total = lax.all_gather(share, "rep", axis=0, tiled=True).astype(jnp.float32)
    updated, new_momentum = step_of(total, params, momentum, replicas)
    return lax.all_gather(updated, "fsdp", axis=0, tiled=True), new_momentum


CORE, CHIP, PLANE = 0, 1, 2


def folded_ring(n):
    return list(range(0, n, 2)) + [i for i in reversed(range(n)) if i % 2] if n > 2 else list(range(n))


def block_of(s, flip_core, flip_chip):
    core = (1 - s[CORE]) if flip_core else s[CORE]
    chip = s[CHIP]
    if flip_chip & 1:
        chip = chip + 1 - 2 * (chip % 2)
    if flip_chip & 2:
        chip = (chip + 2) % 4
    return core * 4 + chip


def pair_kernel(s, mine, theirs, my_scales, their_scales, out):
    a, b = my_scales[...].T, their_scales[...].T
    for k in range(mine.shape[1] // LANES):
        cols = slice(k * LANES, (k + 1) * LANES)
        term = mine[:, cols].astype(jnp.float32) * a[:, k : k + 1]
        term += theirs[:, cols].astype(jnp.float32) * b[:, k : k + 1]
        out[:, cols] = term.astype(out.dtype)


def pair_sum(s, codes, theirs, scales, their_scales, flip, q, dtype):
    width, nblocks = codes.shape[1], scales.shape[0]
    own = lambda i, s: (block_of(s, 0, flip), 0)
    own_t = lambda i, s: (0, block_of(s, 0, flip))
    half = lambda i, s: (block_of(s, 0, flip) - 4 * s[CORE], 0)
    return pl.pallas_call(
        pair_kernel,
        out_shape=jax.ShapeDtypeStruct((q, width), dtype),
        grid_spec=pltpu.PrefetchScalarGridSpec(
            num_scalar_prefetch=1,
            grid=(1,),
            in_specs=[
                pl.BlockSpec((q, width), own),
                pl.BlockSpec((q, width), half),
                pl.BlockSpec((nblocks, q), own_t),
                pl.BlockSpec((nblocks, q), own_t),
            ],
            out_specs=pl.BlockSpec((q, width), lambda i, s: (0, 0)),
        ),
        compiler_params=PARAMS,
        name="pair_sum",
    )(s, codes, theirs, scales, their_scales)


def share_kernel(replicas, s, own, x, y, d, params, momentum, total_out, updated_out):
    total = own[...] + x[...].astype(jnp.float32) + (y[...].astype(jnp.float32) + d[...].astype(jnp.float32))
    total = total.astype(jnp.bfloat16)
    total_out[...] = total
    updated_out[...], _ = step_of(total.astype(jnp.float32), params[...], momentum[...], replicas)


def share_step(s, own, x, y, d, params, momentum, replicas):
    q, width = x.shape
    whole = pl.BlockSpec((q, width), lambda i, s: (0, 0))
    mine = pl.BlockSpec((q, width), lambda i, s: (block_of(s, 0, 0), 0))
    out = jax.ShapeDtypeStruct((q, width), jnp.bfloat16)
    return pl.pallas_call(
        functools.partial(share_kernel, replicas),
        out_shape=(out, out),
        grid_spec=pltpu.PrefetchScalarGridSpec(
            num_scalar_prefetch=1,
            grid=(1,),
            in_specs=[whole] * 4 + [mine] * 2,
            out_specs=(whole, whole),
        ),
        compiler_params=PARAMS,
        name="share_step",
    )(s, own, x, y, d, params, momentum)


def plane_kernel(replicas, s, *refs):
    totals, (params, momentum, updated_out, moment_out) = refs[:8], refs[8:]
    for k, total in enumerate(totals):
        @pl.when(pl.program_id(0) == k)
        def _():
            updated_out[...], moment_out[...] = step_of(
                total[...].astype(jnp.float32), params[...], momentum[...], replicas
            )


def relative_block(i, s):
    core = s[CORE] + (i // 4) * (1 - 2 * s[CORE])
    m = i % 4
    m = jnp.where((core == 0) & (m % 3 != 0), 3 - m, m)
    low = s[CHIP] % 2
    low = low + (m % 2) * (1 - 2 * low)
    high = s[CHIP] // 2
    high = high + (m // 2) * (1 - 2 * high)
    return core * 4 + high * 2 + low


def plane_step(s, totals, params, momentum, planes, replicas):
    q, width = totals[0].shape
    whole = pl.BlockSpec((q, width), lambda i, s: (0, 0))
    block = pl.BlockSpec((q, width), lambda i, s: (relative_block(i, s), 0))
    there = pl.BlockSpec((q, width), lambda i, s: (s[PLANE] * 8 + relative_block(i, s), 0))
    return pl.pallas_call(
        functools.partial(plane_kernel, replicas),
        out_shape=(
            jax.ShapeDtypeStruct((planes * 8 * q, width), jnp.bfloat16),
            jax.ShapeDtypeStruct((8 * q, width), jnp.bfloat16),
        ),
        grid_spec=pltpu.PrefetchScalarGridSpec(
            num_scalar_prefetch=1,
            grid=(8,),
            in_specs=[whole] * 8 + [block] * 2,
            out_specs=(there, block),
        ),
        compiler_params=PARAMS,
        name="plane_step",
    )(s, *totals, params, momentum)


def place_kernel(s, *refs):
    pieces, out = refs[:8], refs[9]
    for k, piece in enumerate(pieces):
        @pl.when(pl.program_id(0) == k)
        def _():
            out[...] = piece[...]


def place(s, pieces, buffer, step):
    q, width = pieces[0].shape
    whole = pl.BlockSpec((q, width), lambda i, s: (0, 0))
    there = pl.BlockSpec((q, width), lambda i, s: (s[PLANE + step] * 8 + relative_block(i, s), 0))
    return pl.pallas_call(
        place_kernel,
        out_shape=jax.ShapeDtypeStruct(buffer.shape, buffer.dtype),
        grid_spec=pltpu.PrefetchScalarGridSpec(
            num_scalar_prefetch=1,
            grid=(8,),
            in_specs=[whole] * 8 + [pl.BlockSpec(memory_space=pl.ANY)],
            out_specs=there,
        ),
        input_output_aliases={9: 0},
        compiler_params=PARAMS,
        name="place",
    )(s, *pieces, buffer)


def eight(codes, block_scales, params, momentum):
    replicas, planes = lax.axis_size("rep"), lax.axis_size("fsdp")
    codes, scales = codes[0], block_scales[0].T
    rows = codes.shape[0]
    half, q = rows // 2, rows // 8

    ring = folded_ring(planes)
    table = np.zeros((replicas * planes, 2 + planes), np.int32)
    for r in range(replicas):
        for z in range(planes):
            at = ring.index(z)
            table[r * planes + z] = [r % 2, r // 2] + [ring[(at - k) % planes] for k in range(planes)]
    me = lax.axis_index("rep") * planes + lax.axis_index("fsdp")
    s = lax.dynamic_index_in_dim(jnp.asarray(table), me, 0, keepdims=False)

    def swap(x, even, odd):
        return lax.ppermute(x, "rep", [(r, r ^ (odd if r % 2 else even)) for r in range(replicas)])

    hop = [(ring[k], ring[(k + 1) % planes]) for k in range(planes)]

    core = lax.axis_index("rep") % 2
    their_scales = swap(scales, 1, 1)
    theirs = swap(lax.dynamic_slice_in_dim(codes, (1 - core) * half, half, 0), 1, 1)

    def pairs(flip, dtype):
        return pair_sum(s, codes, theirs, scales, their_scales, flip, q, dtype)

    from_d = swap(pairs(3, jnp.bfloat16), 6, 6)
    from_x = swap(pairs(1, jnp.bfloat16), 2, 2)
    from_y = swap(pairs(2, jnp.bfloat16), 4, 4)
    total, updated = share_step(s, pairs(0, jnp.float32), from_x, from_y, from_d, params, momentum, replicas)

    def spread(piece):
        first = swap(piece, 4, 2)
        second = swap(piece, 2, 4)
        third = swap(first, 2, 4)
        return [piece, first, second, third]

    pieces = [updated]
    for k in range(planes - 1):
        pieces.append(lax.ppermute(pieces[-1], "fsdp", hop))
    spreads = [spread(total)] + [spread(piece) for piece in pieces[1:]]
    whole = []
    even = lax.axis_index("rep") % 2 == 0
    for piece, first, second, third in spreads:
        got = [piece, first, second, third]
        whole.append(got + [swap(g, 1, 1) for g in got])
    new_params, new_momentum = plane_step(s, whole[0], params, momentum, planes, replicas)
    for k in range(1, planes):
        new_params = place(s, whole[k], new_params, k)
    return new_params, new_momentum


def local(codes, block_scales, params, momentum):
    if lax.axis_size("rep") == 8 and codes.shape[1] % (8 * LANES) == 0:
        return eight(codes, block_scales, params, momentum)
    return general(codes, block_scales, params, momentum)


def solution(mesh):
    return jax.shard_map(
        local,
        mesh=mesh,
        in_specs=(P("rep", "fsdp", None), P("rep", "fsdp", None), P("fsdp", None), P("fsdp", None)),
        out_specs=(P(), P("fsdp", None)),
        check_vma=False,
    )
```

```python
import functools

import jax
import jax.numpy as jnp
from jax import lax
from jax.experimental import pallas as pl
from jax.experimental.pallas import tpu as pltpu
from jax.sharding import PartitionSpec as P


LANES = 128
GRANT = 12 << 20
VMEM = pl.BlockSpec(memory_space=pltpu.VMEM)
ANY = pl.BlockSpec(memory_space=pl.ANY)
HBM = pl.BlockSpec(memory_space=pltpu.HBM)
BF16, F32 = jnp.bfloat16, jnp.float32


def dequantize(code_rows, scale_rows):
    count, width = code_rows.shape
    pieces = code_rows.astype(F32).reshape(count, width // LANES, LANES) * scale_rows[:, :, None]
    return pieces.reshape(count, width)


def step_of(total, params, momentum, replicas):
    delta = total * (1.0 / replicas)
    moment = 0.9 * momentum.astype(F32) + delta
    updated = params.astype(F32) - 0.7 * (delta + 0.9 * moment)
    return updated.astype(BF16), moment.astype(BF16)


def general(codes, block_scales, params, momentum):
    replicas = lax.axis_size("rep")
    term = dequantize(codes[0], block_scales[0]).astype(BF16)
    share = lax.psum_scatter(term, "rep", scatter_dimension=0, tiled=True)
    total = lax.all_gather(share, "rep", axis=0, tiled=True).astype(F32)
    updated, new_momentum = step_of(total, params, momentum, replicas)
    return lax.all_gather(updated, "fsdp", axis=0, tiled=True), new_momentum


class Place:
    def __init__(self, q, mirror=False):
        rep = lax.axis_index("rep")
        core, self.chip = rep % 2, rep // 2
        if mirror:
            core = 1 - core
        self.base = core * (4 * q)
        near, far = 2 - core, 1 + core
        x, y = self.chip % 2, self.chip // 2

        def flip(mask):
            return (x + (mask % 2) * (1 - 2 * x)) + 2 * (y + (mask // 2) * (1 - 2 * y))

        self.own, self.near, self.far, self.both = self.chip, flip(near), flip(far), flip(3)


def folded_ring(n):
    return list(range(0, n, 2)) + [i for i in reversed(range(n)) if i % 2]


def plane_of(step, planes):
    ring, z, out = folded_ring(planes), lax.axis_index("fsdp"), 0
    for at, here in enumerate(ring):
        out = jnp.where(z == here, ring[(at - step) % planes], out)
    return out


def call(kernel, inputs, outputs, specs=None, out_specs=None, scratch=(), aliases=None, grant=GRANT):
    specs = specs or [VMEM] * len(inputs)
    inputs = [pltpu.with_memory_space_constraint(x, pltpu.VMEM) if spec is VMEM else x for x, spec in zip(inputs, specs)]
    return pl.pallas_call(
        kernel,
        out_shape=outputs,
        in_specs=specs,
        out_specs=out_specs or jax.tree.map(lambda _: VMEM, outputs),
        scratch_shapes=list(scratch),
        input_output_aliases=aliases or {},
        compiler_params=pltpu.CompilerParams(vmem_limit_bytes=grant),
    )(*inputs)


def shape(rows, width, dtype=BF16):
    return jax.ShapeDtypeStruct((rows, width), dtype)


def take_kernel(mirror, *refs):
    n = len(refs) // 2 - 1
    (codes, *others), (first, second, *kept), sems = refs[:n], refs[n:-1], refs[-1]
    q = codes.shape[0] // 8
    at, h = Place(q, mirror), q // 2
    copies = [pltpu.make_async_copy(a, b, sems.at[8 + i]) for i, (a, b) in enumerate(zip(others, kept))]
    for i, block in enumerate((at.both, at.far, at.near, at.own)):
        for part, out in enumerate((first, second)):
            start = pl.multiple_of(at.base + block * q + part * h, h)
            copies.append(
                pltpu.make_async_copy(codes.at[pl.ds(start, h)], out.at[pl.ds(i * h, h)], sems.at[2 * i + part])
            )
    for copy in copies:
        copy.start()
    for copy in copies:
        copy.wait()


def take(codes, others, mirror):
    rows, width = codes.shape
    half, n = shape(rows // 4, width), 1 + len(others)
    return call(
functools.partial(take_kernel, mirror),
(codes, *others),
(half, half, *(shape(*x.shape, x.dtype) for x in others)),
[HBM] * n,
scratch=[pltpu.SemaphoreType.DMA((7 + n,))],
    )


def load_kernel(*refs):
    n = len(refs) // 2
    copies = [pltpu.make_async_copy(a, b, refs[-1].at[i]) for i, (a, b) in enumerate(zip(refs[:n], refs[n:-1]))]
    for copy in copies:
        copy.start()
    for copy in copies:
        copy.wait()


def pair_kernel(part, mine, theirs, my_scales, their_scales, sent, near_part, own_part):
    h = mine.shape[0] // 4
    at = Place(2 * h)
    for i, block in enumerate((at.both, at.far, at.near, at.own)):
        cols = pl.ds(pl.multiple_of(at.base + block * 2 * h, 2 * h), 2 * h)
        a = my_scales[:, cols].T[part * h : (part + 1) * h]
        b = their_scales[:, cols].T[part * h : (part + 1) * h]
        rows = slice(i * h, (i + 1) * h)
        for k in range(mine.shape[1] // LANES):
            lanes = slice(k * LANES, (k + 1) * LANES)
            term = mine[rows, lanes].astype(F32) * a[:, k : k + 1] + theirs[rows, lanes].astype(F32) * b[:, k : k + 1]
            if i < 2:
                sent[rows, lanes] = term.astype(BF16)
            elif i == 2:
                near_part[:, lanes] = term
            else:
                own_part[:, lanes] = term


def mid_kernel(near_part, came, out):
    out[...] = (near_part[...] + came[: out.shape[0]].astype(F32)).astype(BF16)


def share_kernel(part, replicas, own, far, near, params, momentum, total_out, updated_out):
    h = own.shape[0]
    at = Place(2 * h)
    rows = pl.ds(pl.multiple_of(at.base + at.own * 2 * h + part * h, h), h)
    total = (own[...] + far[h:].astype(F32) + near[...].astype(F32)).astype(BF16)
    total_out[...] = total
    updated_out[...], _ = step_of(total.astype(F32), params[rows], momentum[rows], replicas)


def update_kernel(which, replicas, total, params, momentum, out):
    q = total.shape[0]
    at = Place(q)
    rows = pl.ds(pl.multiple_of(at.base + getattr(at, which) * q, q), q)
    out[...], _ = step_of(total[...].astype(F32), params[rows], momentum[rows], replicas)


def slots(q):
    for mirror in (False, True):
        at = Place(q, mirror)
        for block in (at.own, at.near, at.far, at.both):
            yield at.base + block * q


def cat_kernel(*refs):
    at = 0
    for ref in refs[:-1]:
        refs[-1][at : at + ref.shape[0]] = ref[...]
        at += ref.shape[0]


def cat(pieces):
    return call(cat_kernel, pieces, shape(sum(x.shape[0] for x in pieces), pieces[0].shape[1]))


def plane_kernel(replicas, planes, q, parts, *refs):
    n = len(refs) - 7
    arrays, (params, momentum, params_out, moment_out, upd, mom, sems) = refs[:n], refs[n:]
    base = plane_of(0, planes) * params.shape[0]
    starts = list(slots(q))
    copies = []
    for k, (array, offset, slot) in enumerate(parts):
        start = pl.multiple_of(starts[slot], q)
        here = pl.ds(start, q)
        total = arrays[array][offset * q : (offset + 1) * q]
        upd[k], mom[k] = step_of(total.astype(F32), params[here], momentum[here], replicas)
        there = pl.ds(pl.multiple_of(base + start, q), q)
        copies.append(pltpu.make_async_copy(upd.at[k], params_out.at[there], sems.at[0, k]))
        copies.append(pltpu.make_async_copy(mom.at[k], moment_out.at[here], sems.at[1, k]))
        copies[-2].start()
        copies[-1].start()
    for copy in copies:
        copy.wait()


def place_kernel(planes, rows, q, parts, *refs):
    out, sems = refs[-2], refs[-1]
    starts = list(slots(q))
    copies = []
    for k, (array, offset, step, slot) in enumerate(parts):
        there = pl.ds(pl.multiple_of(plane_of(step, planes) * rows + starts[slot], q), q)
        piece = refs[array].at[pl.ds(offset * q, q)]
        copies.append(pltpu.make_async_copy(piece, out.at[there], sems.at[k]))
    for copy in copies:
        copy.start()
    for copy in copies:
        copy.wait()


def place(parts, buffer, planes, q):
    arrays = []
    for array, *_ in parts:
        if not any(array is x for x in arrays):
            arrays.append(array)
    n = len(arrays)
    parts = tuple(([x is array for x in arrays].index(True), *rest) for array, *rest in parts)
    return call(
        functools.partial(place_kernel, planes, buffer.shape[0] // planes, q, parts),
        (*arrays, buffer),
        shape(*buffer.shape),
        [VMEM] * n + [ANY],
        ANY,
        [pltpu.SemaphoreType.DMA((len(parts),))],
        {n: 0},
    )


def eight(codes, block_scales, params, momentum):
    replicas, planes = lax.axis_size("rep"), lax.axis_size("fsdp")
    codes, scales = codes[0], block_scales[0].T
    codes, scales, params, momentum = (
        pltpu.with_memory_space_constraint(x, pltpu.HBM) for x in (codes, scales, params, momentum)
    )
    rows, width = codes.shape
    q, h = rows // 8, rows // 16

    def swap(x, even, odd):
        return lax.ppermute(x, "rep", [(r, r ^ (odd if r % 2 else even)) for r in range(replicas)])

    def core(x):
        return swap(x, 1, 1)

    def near(x):
        return swap(x, 4, 2)

    def far(x):
        return swap(x, 2, 4)

    ring = folded_ring(planes)

    def hop(x, step=1):
        return lax.ppermute(x, "fsdp", [(ring[k], ring[(k + step) % planes]) for k in range(planes)])

    their_scales = core(scales)
    sent = take(codes, (), True)
    theirs = [core(x) for x in sent]
    *mine, my_scales = take(codes, (scales,), False)
    params, momentum = call(
        load_kernel, (params, momentum), (shape(rows, width),) * 2, [HBM] * 2, scratch=[pltpu.SemaphoreType.DMA((2,))]
    )
    came, nears, owns = [], [], []
    for i in range(2):
        out, near_part, own_part = call(
            functools.partial(pair_kernel, i),
            (mine[i], theirs[i], my_scales, their_scales),
            (shape(q, width), shape(h, width, F32), shape(h, width, F32)),
        )
        came.append(far(out))
        nears.append(near_part)
        owns.append(own_part)
    last = [near(call(mid_kernel, (nears[i], came[i]), shape(h, width))) for i in range(2)]
    totals, updates = zip(*(
        call(
            functools.partial(share_kernel, i, replicas),
            (owns[i], came[i], last[i], params, momentum),
            (shape(h, width), shape(h, width)),
        )
        for i in range(2)
    ))

    total, updated = cat(totals), cat(updates)
    back1 = hop(updated)
    back2 = hop(back1)
    total_near, total_far = near(total), far(total)

    def update(x, which):
        return call(functools.partial(update_kernel, which, replicas), (x, params, momentum), shape(q, width))

    next_own = hop(updated, -1)
    next_near = hop(update(total_near, "near"), -1)
    next_far = hop(update(total_far, "far"), -1)
    near1, near2 = near(back1), near(back2)
    sent1 = cat((back1, total_near))
    sent2 = cat((back2, near1))
    came1, came2 = far(sent1), far(sent2)
    came3, came4 = far(next_near), far(near2)

    kept = {
        "a": (total, [(0, 0, 0)]),
        "b": (total_far, [(0, 0, 2)]),
        "c": (sent1, [(0, 1, 0), (1, 0, 1)]),
        "d": (came1, [(0, 1, 2), (1, 0, 3)]),
        "e": (sent2, [(0, 2, 0), (1, 1, 1)]),
        "f": (came2, [(0, 2, 2), (1, 1, 3)]),
        "g": (next_own, [(0, 3, 0)]),
        "h": (next_near, [(0, 3, 1)]),
        "i": (next_far, [(0, 3, 2)]),
        "j": (came3, [(0, 3, 3)]),
        "k": (near2, [(0, 2, 1)]),
        "l": (came4, [(0, 2, 3)]),
    }
    twins = {name: core(x) for name, (x, _) in kept.items()}

    def parts_of(names):
        for name in names:
            array, places = kept[name]
            for at, step, slot in places:
                yield array, at, step, slot
                yield twins[name], at, step, slot + 4

    parts = [x for x in parts_of("abcd") if x[2] == 0]
    new_params, new_momentum = call(
        functools.partial(plane_kernel, replicas, planes, q, tuple((i, x[1], x[3]) for i, x in enumerate(parts))),
        (*(x[0] for x in parts), params, momentum),
        (shape(planes * rows, width), shape(rows, width)),
        None,
        (ANY, ANY),
        [pltpu.VMEM((8, q, width), BF16), pltpu.VMEM((8, q, width), BF16), pltpu.SemaphoreType.DMA((2, 8))],
    )
    for names in PLACES:
        parts = [x for x in parts_of(names) if x[2] > 0]
        new_params = place(parts, new_params, planes, q)
    return new_params, new_momentum


PLACES = ("cdefg", "hijk", "l")


def local(codes, block_scales, params, momentum):
    if lax.axis_size("rep") == 8 and lax.axis_size("fsdp") == 4 and codes.shape[1] % (8 * LANES) == 0:
        return eight(codes, block_scales, params, momentum)
    return general(codes, block_scales, params, momentum)


def solution(mesh):
    return jax.shard_map(
        local,
        mesh=mesh,
        in_specs=(P("rep", "fsdp", None), P("rep", "fsdp", None), P("fsdp", None), P("fsdp", None)),
        out_specs=(P(), P("fsdp", None)),
        check_vma=False,
    )
```

```python
import functools

import jax
import jax.numpy as jnp
from jax import lax
from jax.experimental import pallas as pl
from jax.experimental.pallas import tpu as pltpu
from jax.sharding import PartitionSpec as P


LANES = 128
GRANT = 12 << 20
VMEM = pl.BlockSpec(memory_space=pltpu.VMEM)
ANY = pl.BlockSpec(memory_space=pl.ANY)
HBM = pl.BlockSpec(memory_space=pltpu.HBM)
BF16, F32 = jnp.bfloat16, jnp.float32


def dequantize(code_rows, scale_rows):
    count, width = code_rows.shape
    pieces = code_rows.astype(F32).reshape(count, width // LANES, LANES) * scale_rows[:, :, None]
    return pieces.reshape(count, width)


def step_of(total, params, momentum, replicas):
    delta = total * (1.0 / replicas)
    moment = 0.9 * momentum.astype(F32) + delta
    updated = params.astype(F32) - 0.7 * (delta + 0.9 * moment)
    return updated.astype(BF16), moment.astype(BF16)


def general(codes, block_scales, params, momentum):
    replicas = lax.axis_size("rep")
    term = dequantize(codes[0], block_scales[0]).astype(BF16)
    share = lax.psum_scatter(term, "rep", scatter_dimension=0, tiled=True)
    total = lax.all_gather(share, "rep", axis=0, tiled=True).astype(F32)
    updated, new_momentum = step_of(total, params, momentum, replicas)
    return lax.all_gather(updated, "fsdp", axis=0, tiled=True), new_momentum


class Place:
    def __init__(self, q, mirror=False):
        rep = lax.axis_index("rep")
        core, self.chip = rep % 2, rep // 2
        if mirror:
            core = 1 - core
        self.base = core * (4 * q)
        near, far = 2 - core, 1 + core
        x, y = self.chip % 2, self.chip // 2

        def flip(mask):
            return (x + (mask % 2) * (1 - 2 * x)) + 2 * (y + (mask // 2) * (1 - 2 * y))

        self.own, self.near, self.far, self.both = self.chip, flip(near), flip(far), flip(3)


def folded_ring(n):
    return list(range(0, n, 2)) + [i for i in reversed(range(n)) if i % 2]


def plane_of(step, planes):
    ring, z, out = folded_ring(planes), lax.axis_index("fsdp"), 0
    for at, here in enumerate(ring):
        out = jnp.where(z == here, ring[(at - step) % planes], out)
    return out


def call(kernel, inputs, outputs, specs=None, out_specs=None, scratch=(), aliases=None, grant=GRANT):
    specs = specs or [VMEM] * len(inputs)
    inputs = [pltpu.with_memory_space_constraint(x, pltpu.VMEM) if spec is VMEM else x for x, spec in zip(inputs, specs)]
    return pl.pallas_call(
        kernel,
        out_shape=outputs,
        in_specs=specs,
        out_specs=out_specs or jax.tree.map(lambda _: VMEM, outputs),
        scratch_shapes=list(scratch),
        input_output_aliases=aliases or {},
        compiler_params=pltpu.CompilerParams(vmem_limit_bytes=grant),
    )(*inputs)


def shape(rows, width, dtype=BF16):
    return jax.ShapeDtypeStruct((rows, width), dtype)


def take_kernel(mirror, *refs):
    n = len(refs) // 2 - 1
    (codes, *others), (first, second, *kept), sems = refs[:n], refs[n:-1], refs[-1]
    q = codes.shape[0] // 8
    at, h = Place(q, mirror), q // 2
    copies = [pltpu.make_async_copy(a, b, sems.at[8 + i]) for i, (a, b) in enumerate(zip(others, kept))]
    for i, block in enumerate((at.both, at.far, at.near, at.own)):
        for part, out in enumerate((first, second)):
            start = pl.multiple_of(at.base + block * q + part * h, h)
            copies.append(
                pltpu.make_async_copy(codes.at[pl.ds(start, h)], out.at[pl.ds(i * h, h)], sems.at[2 * i + part])
            )
    for copy in copies:
        copy.start()
    for copy in copies:
        copy.wait()


def take(codes, others, mirror):
    rows, width = codes.shape
    half, n = shape(rows // 4, width), 1 + len(others)
    return call(
functools.partial(take_kernel, mirror),
(codes, *others),
(half, half, *(shape(*x.shape, x.dtype) for x in others)),
[HBM] * n,
scratch=[pltpu.SemaphoreType.DMA((7 + n,))],
    )


def load_kernel(*refs):
    n = len(refs) // 2
    copies = [pltpu.make_async_copy(a, b, refs[-1].at[i]) for i, (a, b) in enumerate(zip(refs[:n], refs[n:-1]))]
    for copy in copies:
        copy.start()
    for copy in copies:
        copy.wait()


def pair_kernel(part, mine, theirs, my_scales, their_scales, sent, near_part, own_part):
    h = mine.shape[0] // 4
    at = Place(2 * h)
    for i, block in enumerate((at.both, at.far, at.near, at.own)):
        cols = pl.ds(pl.multiple_of(at.base + block * 2 * h, 2 * h), 2 * h)
        a = my_scales[:, cols].T[part * h : (part + 1) * h]
        b = their_scales[:, cols].T[part * h : (part + 1) * h]
        rows = slice(i * h, (i + 1) * h)
        for k in range(mine.shape[1] // LANES):
            lanes = slice(k * LANES, (k + 1) * LANES)
            term = mine[rows, lanes].astype(F32) * a[:, k : k + 1] + theirs[rows, lanes].astype(F32) * b[:, k : k + 1]
            if i < 2:
                sent[rows, lanes] = term.astype(BF16)
            elif i == 2:
                near_part[:, lanes] = term
            else:
                own_part[:, lanes] = term


def mid_kernel(near_part, came, out):
    out[...] = (near_part[...] + came[: out.shape[0]].astype(F32)).astype(BF16)


def share_kernel(part, replicas, own, far, near, params, momentum, total_out, updated_out):
    h = own.shape[0]
    at = Place(2 * h)
    rows = pl.ds(pl.multiple_of(at.base + at.own * 2 * h + part * h, h), h)
    total = (own[...] + far[h:].astype(F32) + near[...].astype(F32)).astype(BF16)
    total_out[...] = total
    updated_out[...], _ = step_of(total.astype(F32), params[rows], momentum[rows], replicas)


def update_kernel(which, replicas, total, params, momentum, out):
    q = total.shape[0]
    at = Place(q)
    rows = pl.ds(pl.multiple_of(at.base + getattr(at, which) * q, q), q)
    out[...], _ = step_of(total[...].astype(F32), params[rows], momentum[rows], replicas)


def slots(q):
    for mirror in (False, True):
        at = Place(q, mirror)
        for block in (at.own, at.near, at.far, at.both):
            yield at.base + block * q


def cat_kernel(*refs):
    at = 0
    for ref in refs[:-1]:
        refs[-1][at : at + ref.shape[0]] = ref[...]
        at += ref.shape[0]


def cat(pieces):
    return call(cat_kernel, pieces, shape(sum(x.shape[0] for x in pieces), pieces[0].shape[1]))


def plane_kernel(replicas, planes, q, parts, *refs):
    n = len(parts)
    arrays, (params, momentum), (params_out, moment_out, upd, mom, sems) = refs[:n], refs[n : n + 2], refs[-5:]
    base = plane_of(0, planes) * params.shape[0]
    starts = list(slots(q))
    copies = []
    for k, (array, (offset, slot)) in enumerate(zip(arrays, parts)):
        start = pl.multiple_of(starts[slot], q)
        here = pl.ds(start, q)
        total = array[offset * q : (offset + 1) * q]
        upd[k], mom[k] = step_of(total.astype(F32), params[here], momentum[here], replicas)
        there = pl.ds(pl.multiple_of(base + start, q), q)
        copies.append(pltpu.make_async_copy(upd.at[k], params_out.at[there], sems.at[0, k]))
        copies.append(pltpu.make_async_copy(mom.at[k], moment_out.at[here], sems.at[1, k]))
        copies[-2].start()
        copies[-1].start()
    for copy in copies:
        copy.wait()


def plane(parts, params, momentum, out, planes, q, replicas):
    rows, width = params.shape
    n = len(parts)
    return call(
        functools.partial(plane_kernel, replicas, planes, q, tuple((x[1], x[3]) for x in parts)),
        (*(x[0] for x in parts), params, momentum, *out),
        (shape(planes * rows, width), shape(rows, width)),
        [VMEM] * (n + 2) + [ANY] * len(out),
        (ANY, ANY),
        [pltpu.VMEM((n, q, width), BF16), pltpu.VMEM((n, q, width), BF16), pltpu.SemaphoreType.DMA((2, n))],
        {n + 2 + i: i for i in range(len(out))},
    )


def place_kernel(planes, rows, q, parts, *refs):
    out, sems = refs[-2], refs[-1]
    starts = list(slots(q))
    copies = []
    for k, (array, offset, step, slot) in enumerate(parts):
        there = pl.ds(pl.multiple_of(plane_of(step, planes) * rows + starts[slot], q), q)
        piece = refs[array].at[pl.ds(offset * q, q)]
        copies.append(pltpu.make_async_copy(piece, out.at[there], sems.at[k]))
    for copy in copies:
        copy.start()
    for copy in copies:
        copy.wait()


def place(parts, buffer, planes, q):
    arrays = []
    for array, *_ in parts:
        if not any(array is x for x in arrays):
            arrays.append(array)
    n = len(arrays)
    parts = tuple(([x is array for x in arrays].index(True), *rest) for array, *rest in parts)
    return call(
        functools.partial(place_kernel, planes, buffer.shape[0] // planes, q, parts),
        (*arrays, buffer),
        shape(*buffer.shape),
        [VMEM] * n + [ANY],
        ANY,
        [pltpu.SemaphoreType.DMA((len(parts),))],
        {n: 0},
    )


def eight(codes, block_scales, params, momentum):
    replicas, planes = lax.axis_size("rep"), lax.axis_size("fsdp")
    codes, scales = codes[0], block_scales[0].T
    codes, scales, params, momentum = (
        pltpu.with_memory_space_constraint(x, pltpu.HBM) for x in (codes, scales, params, momentum)
    )
    rows, width = codes.shape
    q, h = rows // 8, rows // 16

    def swap(x, even, odd):
        return lax.ppermute(x, "rep", [(r, r ^ (odd if r % 2 else even)) for r in range(replicas)])

    def core(x):
        return swap(x, 1, 1)

    def near(x):
        return swap(x, 4, 2)

    def far(x):
        return swap(x, 2, 4)

    ring = folded_ring(planes)

    def hop(x, step=1):
        return lax.ppermute(x, "fsdp", [(ring[k], ring[(k + step) % planes]) for k in range(planes)])

    their_scales = core(scales)
    sent = take(codes, (), True)
    theirs = [core(x) for x in sent]
    *mine, my_scales = take(codes, (scales,), False)
    params, momentum = call(
        load_kernel, (params, momentum), (shape(rows, width),) * 2, [HBM] * 2, scratch=[pltpu.SemaphoreType.DMA((2,))]
    )
    came, nears, owns = [], [], []
    for i in range(2):
        out, near_part, own_part = call(
            functools.partial(pair_kernel, i),
            (mine[i], theirs[i], my_scales, their_scales),
            (shape(q, width), shape(h, width, F32), shape(h, width, F32)),
        )
        came.append(far(out))
        nears.append(near_part)
        owns.append(own_part)
    last = [near(call(mid_kernel, (nears[i], came[i]), shape(h, width))) for i in range(2)]
    totals, updates = zip(*(
        call(
            functools.partial(share_kernel, i, replicas),
            (owns[i], came[i], last[i], params, momentum),
            (shape(h, width), shape(h, width)),
        )
        for i in range(2)
    ))

    total, updated = cat(totals), cat(updates)
    back1 = cat([hop(x) for x in updates])
    back2 = hop(back1)
    total_near, total_far = near(total), far(total)

    def update(x, which):
        return call(functools.partial(update_kernel, which, replicas), (x, params, momentum), shape(q, width))

    next_own = hop(updated, -1)
    next_near = hop(update(total_near, "near"), -1)
    next_far = hop(update(total_far, "far"), -1)
    near1, near2 = near(back1), near(back2)
    sent1 = cat((back1, total_near))
    sent2 = cat((back2, near1))
    came1, came2 = far(sent1), far(sent2)
    came3, came4 = far(next_near), far(near2)

    kept = {
        "a": (total, [(0, 0, 0)]),
        "b": (total_far, [(0, 0, 2)]),
        "c": (sent1, [(0, 1, 0), (1, 0, 1)]),
        "d": (came1, [(0, 1, 2), (1, 0, 3)]),
        "e": (sent2, [(0, 2, 0), (1, 1, 1)]),
        "f": (came2, [(0, 2, 2), (1, 1, 3)]),
        "g": (next_own, [(0, 3, 0)]),
        "h": (next_near, [(0, 3, 1)]),
        "i": (next_far, [(0, 3, 2)]),
        "j": (came3, [(0, 3, 3)]),
        "k": (near2, [(0, 2, 1)]),
        "l": (came4, [(0, 2, 3)]),
    }
    twins = {name: core(x) for name, (x, _) in kept.items()}

    def parts_of(names):
        for name in names:
            array, places = kept[name]
            for at, step, slot in places:
                yield array, at, step, slot
                yield twins[name], at, step, slot + 4

    out = ()
    for names in PLANE:
        parts = [x for x in parts_of(names) if x[2] == 0]
        out = plane(parts, params, momentum, out, planes, q, replicas)
    new_params, new_momentum = out
    for names in PLACES:
        parts = [x for x in parts_of(names) if x[2] > 0]
        new_params = place(parts, new_params, planes, q)
    return new_params, new_momentum


PLACES = ("cdegh", "fi", "kl", "j")
PLANE = ("abc", "d")


def local(codes, block_scales, params, momentum):
    if lax.axis_size("rep") == 8 and lax.axis_size("fsdp") == 4 and codes.shape[1] % (8 * LANES) == 0:
        return eight(codes, block_scales, params, momentum)
    return general(codes, block_scales, params, momentum)


def solution(mesh):
    return jax.shard_map(
        local,
        mesh=mesh,
        in_specs=(P("rep", "fsdp", None), P("rep", "fsdp", None), P("fsdp", None), P("fsdp", None)),
        out_specs=(P(), P("fsdp", None)),
        check_vma=False,
    )
```
